8 devices in a mesh: dp: 1 (over z), tp: 2 (over y), sp: 4 (over x, core).
Axes of the slice: x: 2, y: 2, z: 1, core: 2. Of those that a mesh axis runs over, the one named last changes fastest.
Arguments:
- hidden: bfloat16 [64, 4096], P('dp')
- norm_gain: float32 [4096], replicated
- w_query: bfloat16 [4096, 4096], P(None, 'tp')
- w_key: bfloat16 [4096, 1024], P(None, 'tp')
- w_value: bfloat16 [4096, 1024], P(None, 'tp')
- w_out: bfloat16 [4096, 4096], P('tp')
- k_cache: bfloat16 [64, 1024, 8, 128], P('dp', 'sp', 'tp')
- v_cache: bfloat16 [64, 1024, 8, 128], P('dp', 'sp', 'tp')
- positions: int32 [64], P('dp')
Outputs:
- output 1: bfloat16 [64, 4096], P('dp')
- output 2: bfloat16 [64, 1024, 8, 128], P('dp', 'sp', 'tp')
- output 3: bfloat16 [64, 1024, 8, 128], P('dp', 'sp', 'tp')
All inputs are finite; a program needn't handle non-finite values.
Results may differ from the reference program's by a relative error of at most 0.00414588.
Values sent between devices are 32-bit elements.
A program may use at most 1 GiB of HBM per device.

```python
import jax
import jax.numpy as jnp
from jax import lax

D = 4096
HEADS = 32
KV_HEADS = 8
HEAD = 128
BATCH = 64
SEQ = 1024
ROPE_BASE = 1000000
EPS = 1e-5
GROUP = HEADS // KV_HEADS


def rotary(tensor, positions):
    half_dim = tensor.shape[-1] // 2
    inv_freq = 1.0 / (ROPE_BASE ** (jnp.arange(half_dim, dtype=jnp.float32) * 2.0 / tensor.shape[-1]))
    angles = positions.astype(jnp.float32)[:, None, None] * inv_freq[None, None, :]
    cosine = jnp.cos(angles)
    sine_val = jnp.sin(angles)
    first_half = tensor[..., :half_dim]
    second_half = tensor[..., half_dim:]
    return jnp.concatenate([first_half * cosine - second_half * sine_val, first_half * sine_val + second_half * cosine], axis=-1)


def smooth_field(base_key, amplitude, noise_scale):
    key_coef, key_noise = jax.random.split(base_key)
    num_freq = 4
    seq_frac = jnp.arange(SEQ, dtype=jnp.float32) / SEQ
    freq_list = jnp.arange(1, num_freq + 1, dtype=jnp.float32)
    phases = 2.0 * jnp.pi * seq_frac[:, None] * freq_list[None, :]
    basis_mat = jnp.concatenate([jnp.cos(phases), jnp.sin(phases)], axis=1)
    coef_mat = jax.random.normal(key_coef, (BATCH, 2 * num_freq, KV_HEADS * HEAD), jnp.float32) * (amplitude / num_freq ** 0.5)
    smooth_part = jnp.einsum("sf,bfc->bsc", basis_mat, coef_mat)
    noise_part = jax.random.normal(key_noise, (BATCH, SEQ, KV_HEADS * HEAD), jnp.float32)
    return (smooth_part + noise_scale * noise_part).reshape(BATCH, SEQ, KV_HEADS, HEAD)


def draw_positions(base_key):
    key_len, key_pick = jax.random.split(base_key)
    pos_draw = jax.random.randint(key_len, (BATCH,), SEQ // 4, SEQ, jnp.int32)
    longest = jax.random.randint(key_pick, (), 0, BATCH, jnp.int32)
    return jnp.where(jnp.arange(BATCH) == longest, SEQ - 1, pos_draw).astype(jnp.int32)


def setup_inputs(seed: int = 0, part: int = 0) -> dict:
    key_list = jax.random.split(jax.random.key(seed), 9)
    q_width = HEADS * HEAD
    kv_width = KV_HEADS * HEAD
    norm_gain = 1.0 + 0.3 * jax.random.normal(key_list[0], (D,), jnp.float32)
    w_query32 = jax.random.normal(key_list[1], (D, q_width), jnp.float32) * D ** -0.5
    head_zero = w_query32.reshape(D, KV_HEADS, GROUP, HEAD)[:, :, 0, :].reshape(D, kv_width)
    w_key32 = 0.75 * head_zero + 0.66 * jax.random.normal(key_list[2], (D, kv_width), jnp.float32) * D ** -0.5
    w_value32 = jax.random.normal(key_list[3], (D, kv_width), jnp.float32) * D ** -0.5
    w_out32 = jax.random.normal(key_list[4], (q_width, D), jnp.float32) * q_width ** -0.5
    hidden = jax.random.normal(jax.random.fold_in(key_list[5], part), (BATCH, D), jnp.float32)
    k_cache = smooth_field(jax.random.fold_in(key_list[6], part), 1.2, 0.5)
    v_cache = smooth_field(jax.random.fold_in(key_list[7], part), 1.5, 0.5)
    positions = draw_positions(jax.random.fold_in(key_list[8], part))
    return {
        "hidden": hidden.astype(jnp.bfloat16),
        "norm_gain": norm_gain,
        "w_query": w_query32.astype(jnp.bfloat16),
        "w_key": w_key32.astype(jnp.bfloat16),
        "w_value": w_value32.astype(jnp.bfloat16),
        "w_out": w_out32.astype(jnp.bfloat16),
        "k_cache": k_cache.astype(jnp.bfloat16),
        "v_cache": v_cache.astype(jnp.bfloat16),
        "positions": positions,
    }


def reference(hidden, norm_gain, w_query, w_key, w_value, w_out, k_cache, v_cache, positions):
    resid_f32 = hidden.astype(jnp.float32)
    normed = (resid_f32 * lax.rsqrt(jnp.mean(resid_f32 * resid_f32, axis=-1, keepdims=True) + EPS) * norm_gain).astype(jnp.bfloat16)
    q_proj = jnp.dot(normed, w_query, preferred_element_type=jnp.float32).reshape(BATCH, HEADS, HEAD)
    k_proj = jnp.dot(normed, w_key, preferred_element_type=jnp.float32).reshape(BATCH, KV_HEADS, HEAD)
    v_new = jnp.dot(normed, w_value, preferred_element_type=jnp.float32).astype(jnp.bfloat16).reshape(BATCH, KV_HEADS, HEAD)
    q_rot = rotary(q_proj, positions).astype(jnp.bfloat16).reshape(BATCH, KV_HEADS, GROUP, HEAD)
    k_new = rotary(k_proj, positions).astype(jnp.bfloat16)
    slot_mask = (jnp.arange(SEQ)[None, :] == positions[:, None])[:, :, None, None]
    k_updated = jnp.where(slot_mask, k_new[:, None], k_cache)
    v_updated = jnp.where(slot_mask, v_new[:, None], v_cache)
    score_scale = HEAD ** -0.5

    def one_sequence(seq_args):
        q_seq, k_seq, v_seq, last_pos = seq_args
        scores = jnp.einsum("kgd,skd->kgs", q_seq.astype(jnp.float32), k_seq.astype(jnp.float32)) * score_scale
        scores = jnp.where(jnp.arange(SEQ) <= last_pos, scores, -jnp.inf)
        attn_prob = jax.nn.softmax(scores, axis=-1)
        return jnp.einsum("kgs,skd->kgd", attn_prob, v_seq.astype(jnp.float32))

    attn_out = lax.map(one_sequence, (q_rot, k_updated, v_updated, positions))
    attn_out = attn_out.astype(jnp.bfloat16).reshape(BATCH, HEADS * HEAD)
    proj_out = jnp.dot(attn_out, w_out, preferred_element_type=jnp.float32)
    return (resid_f32 + proj_out).astype(jnp.bfloat16), k_updated, v_updated
```

```python
import functools
import math

import jax
import jax.numpy as jnp
from jax import lax
from jax.experimental import pallas as pl
from jax.experimental.pallas import tpu as pltpu
from jax.sharding import PartitionSpec as P

ROPE_BASE = 1000000.0
EPS = 1e-5
NEG_BIG = -1e30

B = 64
D = 4096
HD = 128
QL = 16
KVL = 4
SL = 256
RB = SL * KVL
QW, KW = QL * HD, KVL * HD
NW = QW + 2 * KW
WROWS = 256
NWC = D // WROWS
NSLOT = 6
CB = 4
NCC = B // CB
AHEAD = 5
HB = B // 2
STAT = HB * 8 + 8
SCALE = HD ** -0.5 * math.log2(math.e)
F32, BF16 = jnp.float32, jnp.bfloat16
VM = pltpu.VMEM
ANY = pl.ANY


def attn_kernel(pos_ref, hid_ref, gain_ref, cos_ref, sin_ref, wq, wk, wv, kc, vc,
                kout, vout, keep_ref, send_ref,
                wbuf, acc_s, r_s, q_s, kn_s, vn_s, slot_s, ml_s, wsem, ksem, vsem):
    sp = lax.axis_index("sp")
    core = lax.rem(sp, 2)
    off = sp * SL

    def weight_copies(i, slot):
        rows = pl.ds(i * WROWS, WROWS)
        return (
            pltpu.make_async_copy(wq.at[rows], wbuf.at[slot, :, pl.ds(0, QW)], wsem.at[slot, 0]),
            pltpu.make_async_copy(wk.at[rows], wbuf.at[slot, :, pl.ds(QW, KW)], wsem.at[slot, 1]),
            pltpu.make_async_copy(wv.at[rows], wbuf.at[slot, :, pl.ds(QW + KW, KW)], wsem.at[slot, 2]),
        )

    def cache_copies(j):
        rows = pl.ds(j * (CB * RB), CB * RB)
        return (
            pltpu.make_async_copy(kc.at[rows], kout.at[rows], ksem.at[j]),
            pltpu.make_async_copy(vc.at[rows], vout.at[rows], vsem.at[j]),
        )

    def start(copies):
        for c in copies:
            c.start()

    def wait(copies):
        for c in copies:
            c.wait()

    for i in range(NSLOT):
        start(weight_copies(i, i))

    hid = hid_ref[...].astype(F32)
    inv = lax.rsqrt(jnp.mean(hid * hid, axis=-1, keepdims=True) + EPS)
    normed = (hid * inv * gain_ref[...]).astype(BF16)
    for i in range(NWC):
        r_s[i] = normed[:, i * WROWS:(i + 1) * WROWS]
    col = lax.broadcasted_iota(jnp.int32, (QL, RB), 1)
    row = lax.broadcasted_iota(jnp.int32, (QL, RB), 0)
    slot_s[...] = jnp.where(col % KVL == row // (QL // KVL), col // KVL, 1 << 20)
    acc_s[...] = jnp.zeros_like(acc_s)

    def weight_step(i, carry):
        slot = lax.rem(i, NSLOT)
        wait(weight_copies(i, slot))
        acc_s[...] += jnp.dot(r_s[i], wbuf[slot], preferred_element_type=F32)

        @pl.when(i + NSLOT < NWC)
        def _():
            start(weight_copies(i + NSLOT, slot))

        @pl.when(i + NSLOT >= NWC)
        def _():
            start(cache_copies(i + NSLOT - NWC))

        return carry

    lax.fori_loop(0, NWC, weight_step, 0)

    cosf, sinf = cos_ref[...], sin_ref[...]
    for h in range(QL):
        x = acc_s[:, h * HD:(h + 1) * HD]
        q_s[pl.ds(h, B, stride=QL), :] = x * cosf + pltpu.roll(x, HD // 2, 1) * sinf
    for h in range(KVL):
        x = acc_s[:, QW + h * HD:QW + (h + 1) * HD]
        kx = x * cosf + pltpu.roll(x, HD // 2, 1) * sinf
        vx = acc_s[:, QW + KW + h * HD:QW + KW + (h + 1) * HD]
        for t in range(4):
            kn_s[pl.ds(t * KVL + h, B, stride=16), :] = kx
            vn_s[pl.ds(t * KVL + h, B, stride=16), :] = vx

    ml_s[...] = jnp.zeros_like(ml_s)
    lane = lax.broadcasted_iota(jnp.int32, (QL, HD), 1)
    brow = lax.broadcasted_iota(jnp.int32, (16, HD), 0) // KVL

    def cache_step(j, carry):
        @pl.when(j + NSLOT < NCC)
        def _():
            start(cache_copies(j + NSLOT))

        wait(cache_copies(j))
        for t in range(CB):
            b = j * CB + t
            p = pos_ref[b] - off
            base = pl.multiple_of(b * RB, RB)
            pc = jnp.clip(p, 0, SL - 1)
            at = pl.multiple_of(base + (pc // 4) * 16, 16)
            hit = brow == jnp.where((p >= 0) & (p < SL), pc % 4, -1)
            b16 = pl.multiple_of(b * 16, 16)
            kout[pl.ds(at, 16), :] = jnp.where(hit, kn_s[pl.ds(b16, 16), :].astype(BF16), kout[pl.ds(at, 16), :])
            vout[pl.ds(at, 16), :] = jnp.where(hit, vn_s[pl.ds(b16, 16), :].astype(BF16), vout[pl.ds(at, 16), :])
        for t in range(CB):
            b = j * CB + t
            p = pos_ref[b] - off
            base = pl.multiple_of(b * RB, RB)
            b16 = pl.multiple_of(b * 16, 16)
            q = q_s[pl.ds(b16, QL), :].astype(BF16)
            s = lax.dot_general(q, kout[pl.ds(base, RB), :], (((1,), (1,)), ((), ())), preferred_element_type=F32)
            valid = slot_s[...] <= p
            s = jnp.where(valid, s * SCALE, NEG_BIG)
            m = jnp.max(s, axis=-1, keepdims=True)
            e = jnp.where(valid, jnp.exp2(s - m), 0.0)
            l = jnp.sum(e, axis=-1, keepdims=True)
            o = jnp.dot(e.astype(BF16), vout[pl.ds(base, RB), :], preferred_element_type=F32)
            bh, bl = b // HB, lax.rem(b, HB)
            at = pl.ds(pl.multiple_of(bl * 8, 8), 8)
            keep_ref[bh, at, :] = jnp.where(core == 0, o[0:8], o[8:16])
            send_ref[bh, at, :] = jnp.where(core == 0, o[8:16], o[0:8])
            ml = ml_s[...]
            ml = jnp.where(lane == b, m, ml)
            ml_s[...] = jnp.where(lane == b + B, l, ml)
        return carry

    lax.fori_loop(0, NCC, cache_step, 0)
    ml = ml_s[...]
    for bh in range(2):
        keep_ref[bh, pl.ds(HB * 8, 8), :] = jnp.where(core == 0, ml[0:8], ml[8:16])
        send_ref[bh, pl.ds(HB * 8, 8), :] = jnp.where(core == 0, ml[8:16], ml[0:8])


def weights_of(ml_a, ml_b):
    m = jnp.maximum(ml_a, ml_b)
    wa, wb = jnp.exp2(ml_a - m), jnp.exp2(ml_b - m)
    l = wa * pltpu.roll(ml_a, B, 1) + wb * pltpu.roll(ml_b, B, 1)
    return m, l, wa, wb


def merge_kernel(keep_in, recv_in, keep_ref, send_ref):
    chip = lax.axis_index("sp") // 2
    lane = lax.broadcasted_iota(jnp.int32, (8, HD), 1)
    ml = pl.ds(HB * 8, 8)
    m, l, wa, wb = weights_of(keep_in[0, ml, :], recv_in[0, ml, :])
    new = jnp.where(lane < B, m, pltpu.roll(l, B, 1))
    keep_ref[ml, :] = new
    send_ref[ml, :] = new
    for b in range(HB):
        at = pl.ds(b * 8, 8)
        r = []
        for h in range(2):
            c = h * HB + b
            r.append(wa[:, c:c + 1] * keep_in[h, at, :] + wb[:, c:c + 1] * recv_in[h, at, :])
        keep_ref[at, :] = jnp.where(chip == 0, r[0], r[1])
        send_ref[at, :] = jnp.where(chip == 0, r[1], r[0])


def finish_kernel(keep_in, recv_in, o_ref):
    chip = lax.axis_index("sp") // 2
    ml = pl.ds(HB * 8, 8)
    m, l, wa, wb = weights_of(keep_in[ml, :], recv_in[ml, :])
    lane = lax.broadcasted_iota(jnp.int32, (8, HD), 1)
    inv = 1.0 / jnp.where(lane < B, l, 1.0)
    wa, wb = wa * inv, wb * inv
    wa = jnp.where(chip == 0, wa, pltpu.roll(wa, HD - HB, 1))
    wb = jnp.where(chip == 0, wb, pltpu.roll(wb, HD - HB, 1))
    for b in range(HB):
        at = pl.ds(b * 8, 8)
        o = wa[:, b:b + 1] * keep_in[at, :] + wb[:, b:b + 1] * recv_in[at, :]
        o_ref[at, :] = o.astype(BF16).astype(F32)


OC = 8


def out_kernel(own_ref, sib_ref, wo, y0_ref, y1_ref, obuf, lhs, sem):
    core = lax.rem(lax.axis_index("sp"), 2)
    half = QW // 2
    cols = pl.ds(pl.multiple_of(core * (D // 2), D // 2), D // 2)

    def copy(i):
        r0 = jnp.where(i < OC // 2, core, 1 - core) * half + lax.rem(i, OC // 2) * (QW // OC)
        rows = pl.ds(pl.multiple_of(r0, QW // OC), QW // OC)
        return pltpu.make_async_copy(wo.at[rows, cols], obuf.at[i], sem.at[i])

    for i in range(OC):
        copy(i).start()
    for h in range(8):
        lhs[:, h * HD:(h + 1) * HD] = own_ref[pl.ds(h, HB, stride=8), :].astype(BF16)
        lhs[:, half + h * HD:half + (h + 1) * HD] = sib_ref[pl.ds(h, HB, stride=8), :].astype(BF16)
    acc = None
    n = QW // OC
    for i in range(OC):
        copy(i).wait()
        d = jnp.dot(lhs[:, i * n:(i + 1) * n], obuf[i], preferred_element_type=F32)
        acc = d if acc is None else acc + d
    y0_ref[...] = acc[:, :D // 4]
    y1_ref[...] = acc[:, D // 4:]


def write_kernel(src, dst, sem):
    n = src.shape[0] // 8
    copies = [pltpu.make_async_copy(src.at[pl.ds(i * n, n)], dst.at[pl.ds(i * n, n)], sem.at[i]) for i in range(8)]
    for c in copies:
        c.start()
    for c in copies:
        c.wait()


def final_kernel(hid_ref, own0, own1, xr0, xr1, sown0, sown1, sxr0, sxr1, out_ref):
    sp = lax.axis_index("sp")
    chip, core = sp // 2, lax.rem(sp, 2)
    half, quart = D // 2, D // 4
    for mine, parts in ((True, (own0, own1)), (False, (xr0, xr1))):
        rows = pl.ds(pl.multiple_of(jnp.where(chip == 0, 0, HB) if mine else jnp.where(chip == 0, HB, 0), HB), HB)
        for i, part in enumerate(parts):
            cols = pl.ds(pl.multiple_of(core * half + i * quart, quart), quart)
            out_ref[rows, cols] = (hid_ref[rows, cols].astype(F32) + part[...]).astype(BF16)
    for mine, parts in ((True, (sown0, sown1)), (False, (sxr0, sxr1))):
        rows = pl.ds(pl.multiple_of(jnp.where(chip == 0, 0, HB) if mine else jnp.where(chip == 0, HB, 0), HB), HB)
        for i, part in enumerate(parts):
            cols = pl.ds(pl.multiple_of((1 - core) * half + i * quart, quart), quart)
            out_ref[rows, cols] = (hid_ref[rows, cols].astype(F32) + part[...]).astype(BF16)


def cost(us):
    return pl.CostEstimate(flops=int(us * 500e6), bytes_accessed=int(us * 3.3e6), transcendentals=0)


def vspec(n):
    return [pl.BlockSpec(memory_space=VM)] * n


def solution(mesh):
    core_pairs = [(0, 1), (1, 0), (2, 3), (3, 2)]
    chip_pairs = [(0, 2), (2, 0), (1, 3), (3, 1)]
    tp_pairs = [(0, 1), (1, 0)]
    params = lambda mib: pltpu.CompilerParams(vmem_limit_bytes=mib * 2 ** 20)

    def local_step(hidden, norm_gain, w_query, w_key, w_value, w_out, k_cache, v_cache, positions):
        half_dim = HD // 2
        inv_freq = 1.0 / (ROPE_BASE ** (jnp.arange(half_dim, dtype=F32) * 2.0 / HD))
        ang = positions.astype(F32)[:, None] * inv_freq[None, :]
        cosv, sinv = jnp.cos(ang), jnp.sin(ang)
        cosf = jnp.concatenate([cosv, cosv], axis=1)
        sinf = jnp.concatenate([-sinv, sinv], axis=1)

        kvm, vvm, keep0, send0 = pl.pallas_call(
            attn_kernel,
            in_specs=[pl.BlockSpec(memory_space=pltpu.SMEM)] + vspec(4) + [pl.BlockSpec(memory_space=pltpu.HBM)] * 5,
            out_specs=vspec(4),
            out_shape=[VM((B * RB, HD), BF16), VM((B * RB, HD), BF16),
                       VM((2, STAT, HD), F32), VM((2, STAT, HD), F32)],
            scratch_shapes=[
                VM((NSLOT, WROWS, NW), BF16), VM((B, NW), F32), VM((NWC, B, WROWS), BF16),
                VM((B * QL, HD), F32), VM((B * 16, HD), F32), VM((B * 16, HD), F32),
                VM((QL, RB), jnp.int32), VM((QL, HD), F32),
                pltpu.SemaphoreType.DMA((NSLOT, 3)), pltpu.SemaphoreType.DMA((NCC,)), pltpu.SemaphoreType.DMA((NCC,)),
            ],
            compiler_params=params(24),
            cost_estimate=cost(20),
            name="attn",
        )(positions, hidden, norm_gain.reshape(1, D), cosf, sinf, w_query, w_key, w_value,
          k_cache.reshape(B * RB, HD), v_cache.reshape(B * RB, HD))

        def write(x):
            return pl.pallas_call(
                write_kernel, in_specs=vspec(1), out_specs=pl.BlockSpec(memory_space=pltpu.HBM),
                out_shape=jax.ShapeDtypeStruct((B * RB, HD), BF16),
                scratch_shapes=[pltpu.SemaphoreType.DMA((8,))],
                compiler_params=params(4), cost_estimate=cost(5), name="write",
            )(x).reshape(k_cache.shape)

        recv0 = lax.ppermute(send0, "sp", core_pairs)
        keep1, send1 = pl.pallas_call(
            merge_kernel, in_specs=vspec(2), out_specs=vspec(2),
            out_shape=[jax.ShapeDtypeStruct((STAT, HD), F32)] * 2,
            compiler_params=params(4), cost_estimate=cost(0.5), name="merge",
        )(keep0, recv0)
        recv1 = lax.ppermute(send1, "sp", chip_pairs)
        k_out = write(kvm)
        o_own = pl.pallas_call(
            finish_kernel, in_specs=vspec(2), out_specs=vspec(1)[0],
            out_shape=jax.ShapeDtypeStruct((HB * 8, HD), F32),
            compiler_params=params(4), cost_estimate=cost(0.5), name="finish",
        )(keep1, recv1)
        o_sib = lax.ppermute(o_own, "sp", core_pairs)
        y0, y1 = pl.pallas_call(
            out_kernel, in_specs=vspec(2) + [pl.BlockSpec(memory_space=pltpu.HBM)], out_specs=vspec(2),
            out_shape=[jax.ShapeDtypeStruct((HB, D // 4), F32)] * 2,
            scratch_shapes=[VM((OC, QW // OC, D // 2), BF16), VM((HB, QW), BF16), pltpu.SemaphoreType.DMA((OC,))],
            compiler_params=params(12), cost_estimate=cost(3), name="outproj",
        )(o_own, o_sib, pltpu.with_memory_space_constraint(w_out, pltpu.HBM))
        own = [y + lax.ppermute(y, "tp", tp_pairs) for y in (y0, y1)]
        v_out = write(vvm)
        xr = [lax.ppermute(y, "sp", chip_pairs) for y in own]
        sib = [lax.ppermute(y, "sp", core_pairs) for y in own + xr]
        out = pl.pallas_call(
            final_kernel, in_specs=vspec(9), out_specs=vspec(1)[0],
            out_shape=jax.ShapeDtypeStruct((B, D), BF16),
            compiler_params=params(6), cost_estimate=cost(0.5), name="final",
        )(hidden, *own, *xr, *sib)
        return out, k_out, v_out

    cache_spec = P("dp", "sp", "tp", None)
    specs_in = (P("dp", None), P(None), P(None, "tp"), P(None, "tp"), P(None, "tp"), P("tp", None), cache_spec, cache_spec, P("dp"))
    specs_out = (P("dp", None), cache_spec, cache_spec)
    return jax.shard_map(local_step, mesh=mesh, in_specs=specs_in, out_specs=specs_out, check_vma=False)
```
